32 devices in a mesh: row: 2 (over x), col: 16 (over z, y, core).
Axes of the slice: x: 2, y: 2, z: 4, core: 2. Of those that a mesh axis runs over, the one named last changes fastest.
Arguments:
- eigvecs: float32 [16384, 4096], P('row', 'col'), may hold values from -6 to 6
- v_panels: float32 [8, 16384, 256], P(None, 'row', 'col'), as said below
- t_panels: float32 [8, 256, 256], P(None, None, 'col'), as said below
Outputs:
- rotated: float32 [16384, 4096], P('row', 'col')
The draws below stay inside these ranges and needn't reach their ends.
Inputs may be any that keep to these rules, and one draw needn't show every extreme that they name: `v_panels`: in panel k, vector j is zero in rows above k * 256 + j + 1, equals 1 in that row and is dense below it. t_panels[k] is upper triangular and V_k t_panels[k] V_k^T = I minus the product of the panel's 256 Householder reflections, each I - 2 v v^T / (v^T v), taken in the order of j; its diagonal lies in (0, 2].
All inputs are finite; a program needn't handle non-finite values.
Results may differ from the reference program's by a relative error of at most 0.00015.
Values sent between devices are 32-bit elements; how exact they have to be, the bound alone decides.
A program may use at most 192 MiB of HBM per device.

```python
import math
import jax
import jax.numpy as jnp
from jax import lax

ORDER = 16384
PANEL_W = 256
PANELS = 8
COLS = 4096


def householder_panels(key):
    noise = jax.random.normal(jax.random.fold_in(key, 7), (PANELS, ORDER, PANEL_W), jnp.float32) / math.sqrt(ORDER)
    rows_at = lax.broadcasted_iota(jnp.int32, (PANELS, ORDER, PANEL_W), 1)
    column_at = lax.broadcasted_iota(jnp.int32, (PANELS, ORDER, PANEL_W), 2)
    panel_at = lax.broadcasted_iota(jnp.int32, (PANELS, ORDER, PANEL_W), 0)
    unit_row = panel_at * PANEL_W + column_at + 1
    return jnp.where(rows_at > unit_row, noise, jnp.where(rows_at == unit_row, 1.0, 0.0)).astype(jnp.float32)


def draw_v_panels(key, part):
    return householder_panels(key)


def draw_t_panels(key, part):
    vectors = householder_panels(key)
    gram = jnp.einsum('knb,knc->kbc', vectors, vectors, precision=lax.Precision.HIGHEST)
    identity = jnp.eye(PANEL_W, dtype=jnp.float32)
    inverse_factor = jnp.triu(gram, 1) + 0.5 * gram * identity
    eye_stack = jnp.broadcast_to(identity, (PANELS, PANEL_W, PANEL_W))
    factor = lax.linalg.triangular_solve(inverse_factor, eye_stack, left_side=True, lower=False)
    return jnp.triu(factor).astype(jnp.float32)


def block_scale(own_key, shape, split, least, largest):
    level = 1.0
    for position, shards_of in split:
        draws = jax.random.uniform(jax.random.fold_in(jax.random.fold_in(own_key, 6), position), (shards_of,), jnp.float32, least / len(split), largest / len(split))
        level = level * jnp.repeat(jnp.exp(draws), shape[position] // shards_of).reshape((-1,) + (1,) * (len(shape) - 1 - position))
    return level


def scatter_about(rng, shape, deviation, most, pieces=(), held_as=jnp.bfloat16):
    loudness = block_scale(rng, shape, pieces, -0.22, 0.18) if pieces else 1.0
    drawn = jax.random.normal(rng, shape, jnp.float32) * deviation * loudness
    return jnp.minimum(jnp.maximum(drawn, -most), most).astype(held_as)


def setup_inputs(seed: int = 0) -> dict:
    keys = jax.random.split(jax.random.key(seed), 4)
    return {
        "eigvecs": scatter_about(keys[0], (ORDER, COLS), 1.0, 6.0, ((0, 2), (1, 16)), jnp.float32),
        "v_panels": draw_v_panels(jax.random.fold_in(keys[3], 71), 0),
        "t_panels": draw_t_panels(jax.random.fold_in(keys[3], 71), 0),
    }


def reference(eigvecs, v_panels, t_panels):
    current = eigvecs
    for panel_index in reversed(range(PANELS)):
        vectors = v_panels[panel_index]
        projected = jnp.dot(vectors.T.astype(jnp.float32), current.astype(jnp.float32), preferred_element_type=jnp.float32, precision=lax.Precision.HIGHEST)
        scaled = jnp.dot(t_panels[panel_index].astype(jnp.float32), projected.astype(jnp.float32), preferred_element_type=jnp.float32, precision=lax.Precision.HIGHEST)
        current = current - jnp.dot(vectors.astype(jnp.float32), scaled.astype(jnp.float32), preferred_element_type=jnp.float32, precision=lax.Precision.HIGHEST)
    return current
```

```python
import functools

import jax
import jax.numpy as jnp
from jax import lax
from jax.experimental import pallas as pl
from jax.experimental.pallas import tpu as pltpu
from jax.sharding import PartitionSpec as P

SLOTS = 4
MESH = pl.DeviceIdType.MESH


def halves(x):
    high = x.astype(jnp.bfloat16)
    return high, (x - high.astype(jnp.float32)).astype(jnp.bfloat16)


def dot3(left, right, left_axis, right_axis):
    def one(a, b):
        return lax.dot_general(
            a, b, (((left_axis,), (right_axis,)), ((), ())), preferred_element_type=jnp.float32
        )

    (lh, ll), (rh, rl) = left, right
    return one(lh, rh) + (one(ll, rh) + one(lh, rl))


def kernel(shape, z_hbm, p_ref, out_ref, g_ref, zbuf, vbuf, acc, psend, precv, *sems):
    panels, width, rows, groups, A, B = shape
    recv, su, sd, sy, sc, lsem, zsem, psnd, prcv = sems
    per = p_ref.shape[1]
    length = p_ref.shape[2]
    tiles = length // 128
    cut = (tiles - tiles // 6) * 128
    lanes = (pl.ds(0, cut), pl.ds(cut, length - cut))
    tile = min(rows, 1024)
    me = lax.axis_index("col")
    my_row = lax.axis_index("row")
    c = lax.rem(me, 2)
    b = lax.rem(me // 2, B)
    a = me // (2 * B)

    def index(aa, bb, cc):
        return (aa * B + bb) * 2 + cc

    def walk(i, s, go):
        k = panels - 1 - i
        sl = lax.rem(i, SLOTS)

        def place(owner, q):
            return g_ref.at[k, pl.ds(pl.multiple_of(owner * per, per), per), lanes[q]]

        def move(owner, q, own, target, sem):
            copy = pltpu.make_async_remote_copy(
                src_ref=p_ref.at[k, :, lanes[q]] if own else place(owner, q),
                dst_ref=place(owner, q),
                send_sem=sem,
                recv_sem=recv.at[sl, q, owner],
                device_id={"col": target},
                device_id_type=MESH,
            )
            if go:
                copy.start()
            else:
                copy.wait_send()

        def arrive(owner, q):
            if go:
                pltpu.make_async_remote_copy(
                    src_ref=place(owner, q),
                    dst_ref=place(owner, q),
                    send_sem=sc.at[sl, q, 0],
                    recv_sem=recv.at[sl, q, owner],
                    device_id={"col": index(a, b, 1 - c)},
                    device_id_type=MESH,
                ).wait_recv()

        def along(sg, owner, q, own, cid):
            if sg >= 0:

                @pl.when(a < A - 1)
                def _():
                    move(owner, q, own, index(a + 1, b, c), su.at[sl, q, cid])

            if sg <= 0:

                @pl.when(a > 0)
                def _():
                    move(owner, q, own, index(a - 1, b, c), sd.at[sl, q, cid])

        def across(owner, q, own, slot):
            for j in range(1, B):
                move(owner, q, own, index(a, lax.rem(b + j, B), c), sy.at[sl, slot, j - 1])

        def over(owner, q, own, cid):
            move(owner, q, own, index(a, b, 1 - c), sc.at[sl, q, cid])

        def signs(d):
            return (1, -1) if d else (0,)

        if s < A:
            for sg in signs(s):
                at = a - sg * s

                @pl.when((at >= 0) & (at < A))
                def _(sg=sg, at=at):
                    owner, cid, own = index(at, b, c), at * B + b, s == 0
                    if not own:
                        arrive(owner, 0)
                    along(sg, owner, 0, own, cid)
                    across(owner, 0, own, at)
                    over(owner, 0, own, cid)

        if s == 0:
            across(me, 1, True, A)
            along(0, me, 1, True, a * B + b)
            over(me, 1, True, a * B + b)
        else:
            for sg in signs(s - 1):
                at = a - sg * (s - 1)

                @pl.when((at >= 0) & (at < A))
                def _(sg=sg, at=at):
                    for j in range(B):
                        if s == 1 and j == 0:
                            continue
                        bb = lax.rem(b + j, B)
                        owner, cid = index(at, bb, c), at * B + bb
                        arrive(owner, 1)
                        along(sg, owner, 1, False, cid)
                        over(owner, 1, False, cid)
                    for j in range(1, B):
                        bb = lax.rem(b + j, B)
                        owner, cid = index(at, bb, c), at * B + bb
                        arrive(owner, 0)
                        over(owner, 0, False, cid)

    def settle(i):
        k = panels - 1 - i
        sl = lax.rem(i, SLOTS)
        for at in range(A):
            for bb in range(B):
                owner = index(at, bb, 1 - c)
                for q in range(2):
                    spot = g_ref.at[k, pl.ds(pl.multiple_of(owner * per, per), per), lanes[q]]
                    pltpu.make_async_remote_copy(
                        src_ref=spot,
                        dst_ref=spot,
                        send_sem=sc.at[sl, q, 0],
                        recv_sem=recv.at[sl, q, owner],
                        device_id={"col": index(a, b, 1 - c)},
                        device_id_type=MESH,
                    ).wait_recv()

    def load(i):
        k = panels - 1 - i
        sl = lax.rem(i, 2)
        for owner in range(A * B * 2):
            spot = pl.ds(owner * per, per)

            @pl.when(me == owner)
            def _():
                pltpu.make_async_copy(p_ref.at[k], vbuf.at[sl, spot], lsem.at[sl]).start()

            @pl.when(me != owner)
            def _():
                pltpu.make_async_copy(g_ref.at[k, spot], vbuf.at[sl, spot], lsem.at[sl]).start()

    def partial(sl, j):
        return pltpu.make_async_remote_copy(
            src_ref=psend.at[sl],
            dst_ref=precv.at[sl, j - 1],
            send_sem=psnd.at[sl, j - 1],
            recv_sem=prcv.at[sl, j - 1],
            device_id={"row": lax.rem(my_row + j, groups)},
            device_id_type=MESH,
        )

    def project(i):
        k = panels - 1 - i
        sl = lax.rem(i, 2)
        pltpu.make_async_copy(g_ref.at[k], vbuf.at[sl], lsem.at[sl]).wait()
        acc[...] = jnp.zeros_like(acc)

        def body(n, _):
            at = pl.multiple_of(n * tile, tile)
            left = halves(vbuf[sl, :, pl.ds(at, tile)])
            right = halves(zbuf[pl.ds(at, tile), :])
            acc[...] += dot3(left, right, 1, 0)
            return 0

        lax.fori_loop(0, rows // tile, body, 0)
        psend[sl] = acc[...]
        for j in range(1, groups):
            partial(sl, j).start()

    def update(i):
        sl = lax.rem(i, 2)
        total = acc[...]
        for j in range(1, groups):
            partial(sl, j).wait()
            total = total + precv[sl, j - 1]
        factor = halves(vbuf[sl, :, pl.ds(rows, width)])
        scaled = halves(dot3(factor, halves(total), 0, 0))

        def body(n, _):
            at = pl.multiple_of(n * tile, tile)
            left = halves(vbuf[sl, :, pl.ds(at, tile)])
            zbuf[pl.ds(at, tile), :] = zbuf[pl.ds(at, tile), :] - dot3(left, scaled, 0, 0)
            return 0

        lax.fori_loop(0, rows // tile, body, 0)

    fetch = pltpu.make_async_copy(z_hbm, zbuf, zsem)
    fetch.start()
    walk(0, 0, True)
    fetch.wait()

    def iteration(i, _):
        @pl.when(i > 0)
        def _():
            walk(i - 1, A, True)
            settle(i - 1)
            load(i - 1)

        @pl.when(i < panels)
        def _():
            walk(i, 1, True)

        @pl.when(i > 0)
        def _():
            project(i - 1)

        @pl.when(i + 1 < panels)
        def _():
            walk(i + 1, 0, True)

        @pl.when(i < panels)
        def _():
            for s in range(2, A - 1):
                walk(i, s, True)

        @pl.when(i > 0)
        def _():
            update(i - 1)

        @pl.when(i < panels)
        def _():
            walk(i, A - 1, True)

        @pl.when(i > 0)
        def _():
            for s in range(A + 1):
                walk(i - 1, s, False)

        return 0

    lax.fori_loop(0, panels + 1, iteration, 0)
    store = pltpu.make_async_copy(zbuf, out_ref, zsem)
    store.start()
    store.wait()


def local(eigvecs, v_panels, t_panels):
    panels, rows, per = v_panels.shape
    width = t_panels.shape[1]
    groups = lax.axis_size("row")
    members = lax.axis_size("col")
    chips = members // 2
    B = max(n for n in range(1, chips + 1) if chips % n == 0 and n * n <= chips)
    A = chips // B
    columns = eigvecs.shape[1]
    packed = jnp.concatenate(
        [jnp.transpose(v_panels, (0, 2, 1)), jnp.transpose(t_panels, (0, 2, 1))], axis=2
    )
    length = rows + width
    dma = pltpu.SemaphoreType.DMA
    anywhere = pl.BlockSpec(memory_space=pl.ANY)
    others = max(groups - 1, 1)
    out, _ = pl.pallas_call(
        functools.partial(kernel, (panels, width, rows, groups, A, B)),
        out_shape=(
            jax.ShapeDtypeStruct((rows, columns), jnp.float32),
            jax.ShapeDtypeStruct((panels, width, length), jnp.float32),
        ),
        in_specs=[anywhere] * 2,
        out_specs=(anywhere, anywhere),
        scratch_shapes=[
            pltpu.VMEM((rows, columns), jnp.float32),
            pltpu.VMEM((2, width, length), jnp.float32),
            pltpu.VMEM((width, columns), jnp.float32),
            pltpu.VMEM((2, width, columns), jnp.float32),
            pltpu.VMEM((2, others, width, columns), jnp.float32),
            dma((SLOTS, 2, members)),
            dma((SLOTS, 2, chips)),
            dma((SLOTS, 2, chips)),
            dma((SLOTS, A + 1, max(B - 1, 1))),
            dma((SLOTS, 2, chips)),
            dma((2,)),
            dma,
            dma((2, others)),
            dma((2, others)),
        ],
        compiler_params=pltpu.CompilerParams(has_side_effects=True, vmem_limit_bytes=60 * 2**20),
    )(eigvecs, packed)
    return out


def solution(mesh):
    in_specs = (P("row", "col"), P(None, "row", "col"), P(None, None, "col"))
    out_specs = P("row", "col")
    return jax.shard_map(local, mesh=mesh, in_specs=in_specs, out_specs=out_specs, check_vma=False)
```

```python
import functools

import jax
import jax.numpy as jnp
from jax import lax
from jax.experimental import pallas as pl
from jax.experimental.pallas import tpu as pltpu
from jax.sharding import PartitionSpec as P

SLOTS = 4
MESH = pl.DeviceIdType.MESH


def halves(x):
    high = x.astype(jnp.bfloat16)
    return high, (x - high.astype(jnp.float32)).astype(jnp.bfloat16)


def dot3(left, right, left_axis, right_axis):
    def one(a, b):
        return lax.dot_general(
            a, b, (((left_axis,), (right_axis,)), ((), ())), preferred_element_type=jnp.float32
        )

    (lh, ll), (rh, rl) = left, right
    return one(lh, rh) + (one(ll, rh) + one(lh, rl))


def kernel(shape, z_hbm, p_ref, out_ref, g_ref, zbuf, vbuf, acc, psend, precv, *sems):
    panels, width, rows, groups, A, B = shape
    recv, su, sd, sy, sc, lsem, zsem, psnd, prcv = sems
    per = p_ref.shape[1]
    length = p_ref.shape[2]
    tiles = length // 128
    cut = (tiles - tiles // 4) * 128
    lanes = (pl.ds(0, cut), pl.ds(cut, length - cut))
    tile = min(rows, 1024)
    me = lax.axis_index("col")
    my_row = lax.axis_index("row")
    c = lax.rem(me, 2)
    b = lax.rem(me // 2, B)
    a = me // (2 * B)

    def index(aa, bb, cc):
        return (aa * B + bb) * 2 + cc

    def walk(i, s, go):
        k = panels - 1 - i
        sl = lax.rem(i, SLOTS)

        def place(owner, q):
            return g_ref.at[k, pl.ds(pl.multiple_of(owner * per, per), per), lanes[q]]

        def move(owner, q, own, target, sem):
            copy = pltpu.make_async_remote_copy(
                src_ref=p_ref.at[k, :, lanes[q]] if own else place(owner, q),
                dst_ref=place(owner, q),
                send_sem=sem,
                recv_sem=recv.at[sl, q, owner],
                device_id={"col": target},
                device_id_type=MESH,
            )
            if go:
                copy.start()
            else:
                copy.wait_send()

        def arrive(owner, q):
            if go:
                pltpu.make_async_remote_copy(
                    src_ref=place(owner, q),
                    dst_ref=place(owner, q),
                    send_sem=sc.at[sl, q, 0],
                    recv_sem=recv.at[sl, q, owner],
                    device_id={"col": index(a, b, 1 - c)},
                    device_id_type=MESH,
                ).wait_recv()

        def along(sg, owner, q, own, cid):
            if sg >= 0:

                @pl.when(a < A - 1)
                def _():
                    move(owner, q, own, index(a + 1, b, c), su.at[sl, q, cid])

            if sg <= 0:

                @pl.when(a > 0)
                def _():
                    move(owner, q, own, index(a - 1, b, c), sd.at[sl, q, cid])

        def across(owner, q, own, slot):
            for j in range(1, B):
                move(owner, q, own, index(a, lax.rem(b + j, B), c), sy.at[sl, slot, j - 1])

        def over(owner, q, own, cid):
            move(owner, q, own, index(a, b, 1 - c), sc.at[sl, q, cid])

        def signs(d):
            return (1, -1) if d else (0,)

        if s < A:
            for sg in signs(s):
                at = a - sg * s

                @pl.when((at >= 0) & (at < A))
                def _(sg=sg, at=at):
                    owner, cid, own = index(at, b, c), at * B + b, s == 0
                    if not own:
                        arrive(owner, 0)
                    along(sg, owner, 0, own, cid)
                    across(owner, 0, own, at)
                    over(owner, 0, own, cid)

        if s == 0:
            across(me, 1, True, A)
            along(0, me, 1, True, a * B + b)
            over(me, 1, True, a * B + b)
        else:
            for sg in signs(s - 1):
                at = a - sg * (s - 1)

                @pl.when((at >= 0) & (at < A))
                def _(sg=sg, at=at):
                    for j in range(B):
                        if s == 1 and j == 0:
                            continue
                        bb = lax.rem(b + j, B)
                        owner, cid = index(at, bb, c), at * B + bb
                        arrive(owner, 1)
                        along(sg, owner, 1, False, cid)
                        over(owner, 1, False, cid)
                    for j in range(1, B):
                        bb = lax.rem(b + j, B)
                        owner, cid = index(at, bb, c), at * B + bb
                        arrive(owner, 0)
                        over(owner, 0, False, cid)

    def settle(i):
        k = panels - 1 - i
        sl = lax.rem(i, SLOTS)
        for at in range(A):
            for bb in range(B):
                owner = index(at, bb, 1 - c)
                for q in range(2):
                    spot = g_ref.at[k, pl.ds(pl.multiple_of(owner * per, per), per), lanes[q]]
                    pltpu.make_async_remote_copy(
                        src_ref=spot,
                        dst_ref=spot,
                        send_sem=sc.at[sl, q, 0],
                        recv_sem=recv.at[sl, q, owner],
                        device_id={"col": index(a, b, 1 - c)},
                        device_id_type=MESH,
                    ).wait_recv()

    def load(i):
        k = panels - 1 - i
        sl = lax.rem(i, 2)
        for owner in range(A * B * 2):
            spot = pl.ds(owner * per, per)

            @pl.when(me == owner)
            def _():
                pltpu.make_async_copy(p_ref.at[k], vbuf.at[sl, spot], lsem.at[sl]).start()

            @pl.when(me != owner)
            def _():
                pltpu.make_async_copy(g_ref.at[k, spot], vbuf.at[sl, spot], lsem.at[sl]).start()

    def partial(sl, j):
        return pltpu.make_async_remote_copy(
            src_ref=psend.at[sl],
            dst_ref=precv.at[sl, j - 1],
            send_sem=psnd.at[sl, j - 1],
            recv_sem=prcv.at[sl, j - 1],
            device_id={"row": lax.rem(my_row + j, groups)},
            device_id_type=MESH,
        )

    def project(i):
        k = panels - 1 - i
        sl = lax.rem(i, 2)
        pltpu.make_async_copy(g_ref.at[k], vbuf.at[sl], lsem.at[sl]).wait()
        acc[...] = jnp.zeros_like(acc)

        def body(n, _):
            at = pl.multiple_of(n * tile, tile)
            left = halves(vbuf[sl, :, pl.ds(at, tile)])
            right = halves(zbuf[pl.ds(at, tile), :])
            acc[...] += dot3(left, right, 1, 0)
            return 0

        lax.fori_loop(0, rows // tile, body, 0)
        psend[sl] = acc[...]
        for j in range(1, groups):
            partial(sl, j).start()

    def store(n):
        spot = pl.ds(pl.multiple_of(n * tile, tile), tile)
        return pltpu.make_async_copy(zbuf.at[spot], out_ref.at[spot], zsem)

    def update(i):
        sl = lax.rem(i, 2)
        total = acc[...]
        for j in range(1, groups):
            partial(sl, j).wait()
            total = total + precv[sl, j - 1]
        factor = halves(vbuf[sl, :, pl.ds(rows, width)])
        scaled = halves(dot3(factor, halves(total), 0, 0))

        def body(n, _):
            at = pl.multiple_of(n * tile, tile)
            left = halves(vbuf[sl, :, pl.ds(at, tile)])
            zbuf[pl.ds(at, tile), :] = zbuf[pl.ds(at, tile), :] - dot3(left, scaled, 0, 0)

            @pl.when((i == panels - 1) & (n > 0))
            def _():
                store(n - 1).start()

            return 0

        lax.fori_loop(0, rows // tile, body, 0)

    fetch = pltpu.make_async_copy(z_hbm, zbuf, zsem)
    fetch.start()
    walk(0, 0, True)
    fetch.wait()

    def iteration(i, _):
        @pl.when(i < panels)
        def _():
            walk(i, 1, True)

        @pl.when(i > 0)
        def _():
            walk(i - 1, A, True)

        @pl.when(i + 1 < panels)
        def _():
            walk(i + 1, 0, True)

        @pl.when(i > 0)
        def _():
            settle(i - 1)
            load(i - 1)

        @pl.when(i < panels)
        def _():
            for s in range(2, A - 1):
                walk(i, s, True)

        @pl.when(i > 0)
        def _():
            project(i - 1)

        @pl.when(i < panels)
        def _():
            walk(i, A - 1, True)

        @pl.when(i > 0)
        def _():
            update(i - 1)

        @pl.when(i > 0)
        def _():
            for s in range(A + 1):
                walk(i - 1, s, False)

        return 0

    lax.fori_loop(0, panels + 1, iteration, 0)
    store(rows // tile - 1).start()
    pltpu.make_async_copy(zbuf, out_ref, zsem).wait()


def local(eigvecs, v_panels, t_panels):
    panels, rows, per = v_panels.shape
    width = t_panels.shape[1]
    groups = lax.axis_size("row")
    members = lax.axis_size("col")
    chips = members // 2
    B = max(n for n in range(1, chips + 1) if chips % n == 0 and n * n <= chips)
    A = chips // B
    columns = eigvecs.shape[1]
    packed = jnp.concatenate(
        [jnp.transpose(v_panels, (0, 2, 1)), jnp.transpose(t_panels, (0, 2, 1))], axis=2
    )
    length = rows + width
    dma = pltpu.SemaphoreType.DMA
    anywhere = pl.BlockSpec(memory_space=pl.ANY)
    others = max(groups - 1, 1)
    out, _ = pl.pallas_call(
        functools.partial(kernel, (panels, width, rows, groups, A, B)),
        out_shape=(
            jax.ShapeDtypeStruct((rows, columns), jnp.float32),
            jax.ShapeDtypeStruct((panels, width, length), jnp.float32),
        ),
        in_specs=[anywhere] * 2,
        out_specs=(anywhere, anywhere),
        scratch_shapes=[
            pltpu.VMEM((rows, columns), jnp.float32),
            pltpu.VMEM((2, width, length), jnp.float32),
            pltpu.VMEM((width, columns), jnp.float32),
            pltpu.VMEM((2, width, columns), jnp.float32),
            pltpu.VMEM((2, others, width, columns), jnp.float32),
            dma((SLOTS, 2, members)),
            dma((SLOTS, 2, chips)),
            dma((SLOTS, 2, chips)),
            dma((SLOTS, A + 1, max(B - 1, 1))),
            dma((SLOTS, 2, chips)),
            dma((2,)),
            dma,
            dma((2, others)),
            dma((2, others)),
        ],
        compiler_params=pltpu.CompilerParams(has_side_effects=True, vmem_limit_bytes=60 * 2**20),
    )(eigvecs, packed)
    return out


def solution(mesh):
    in_specs = (P("row", "col"), P(None, "row", "col"), P(None, None, "col"))
    out_specs = P("row", "col")
    return jax.shard_map(local, mesh=mesh, in_specs=in_specs, out_specs=out_specs, check_vma=False)
```
